256 devices in a mesh: img: 4 (over y_hi, core), txt: 64 (over x, y_lo, z).
Axes of the slice: x: 4, y: 4 (y_hi: 2, y_lo: 2; y = y_hi * 2 + y_lo), z: 8, core: 2. Of those that a mesh axis runs over, the one named last changes fastest.
Arguments:
- queries: bfloat16 [1, 40960, 8192], P(None, 'txt', 'img'), may hold values from -128 to 128
- visual_keys: bfloat16 [1, 512, 8192], P(None, 'img'), may hold values from -5 to 5
- visual_values: bfloat16 [1, 512, 8192], P(None, 'img'), may hold values from -6 to 6
- out_grad: bfloat16 [1, 40960, 8192], P(None, 'txt', 'img'), may hold values from -6 to 6
- gate_value: float32 [1, 64], P(None, 'img'), may hold values from -1.5 to 1.5
- image_order: int32 [1, 8], replicated, may hold values from 0 to 7, as said below
- image_seen: int32 [40960], P('txt'), may hold values from 1 to 8
Outputs:
- query_grad: bfloat16 [1, 40960, 8192], P(None, 'txt', 'img')
- key_grad: float32 [1, 512, 8192], P(None, 'txt', 'img')
- value_grad: float32 [1, 512, 8192], P(None, 'txt', 'img')
The draws below stay inside these ranges and needn't reach their ends.
Inputs may be any that keep to these rules, and one draw needn't show every extreme that they name: `image_order`: each row names every image of 0 to 7 once.
All inputs are finite; a program needn't handle non-finite values.
Results may differ from the reference program's by a relative error of at most 0.0058.
Values may be sent and summed in bfloat16 or wider, within the bound.
No kernel may reach another device: no remote copies, remote signals or barrier semaphores. Data moves between devices by JAX's collectives and lax.ppermute only.
A program may use at most 128 MiB of HBM per device.

```python
import math
import jax
import jax.numpy as jnp
from jax import lax

D = 8192
H = 64
HD = 128
LAT = 64
IMAGES = 8
LAYERS = 1
TOK_DEV = 640
TOKENS = 40960
KEYS = 512


def order_table(key):
    row_list = [jax.random.permutation(jax.random.fold_in(key, 100 + layer_index), IMAGES) for layer_index in range(LAYERS)]
    return jnp.stack(row_list).astype(jnp.int32)


def key_table(key):
    normal_table = jnp.clip(jax.random.normal(jax.random.fold_in(key, 7), (LAYERS, KEYS, D), jnp.float32), -5.0, 5.0)
    return normal_table


def draw_image_order(key, part):
    return order_table(key)


def draw_visual_keys(key, part):
    return key_table(key).astype(jnp.bfloat16)


def draw_queries(key, part):
    normal_table = jnp.clip(jax.random.normal(jax.random.fold_in(key, 9), (LAYERS, TOKENS, D), jnp.float32), -5.0, 5.0)
    return normal_table.astype(jnp.bfloat16)


def set_ends(drawn, stream_key, low, largest):
    spot = [jax.random.randint(jax.random.fold_in(stream_key, axis), (), 0, length) for axis, length in enumerate(drawn.shape)]
    widest = drawn.shape.index(max(drawn.shape))
    neighbour = spot[:widest] + [(spot[widest] + 1) % drawn.shape[widest]] + spot[widest + 1:]
    return drawn.at[tuple(spot)].set(low).at[tuple(neighbour)].set(largest)


def shard_levels(rng, dims, split, least, largest):
    def one(dim, shards_of):
        heights = jax.random.uniform(jax.random.fold_in(jax.random.fold_in(rng, 6), dim), (shards_of,), jnp.float32, least / len(split), largest / len(split))
        return jnp.repeat(jnp.exp(heights), dims[dim] // shards_of).reshape((-1,) + (1,) * (len(dims) - dim - 1))

    level = one(*split[0])
    for cut in split[1:]:
        level = level * one(*cut)
    return level


def scatter_about(stream_key, extent, width, most, shards=(), dtype=jnp.bfloat16):
    gain = shard_levels(stream_key, extent, shards, -0.22, 0.18) if shards else 1.0
    entries = jax.random.normal(stream_key, extent, jnp.float32) * width * gain
    return jnp.minimum(jnp.maximum(entries, -most), most).astype(dtype)


def setup_inputs(seed: int = 0) -> dict:
    streams_of = jax.random.split(jax.random.key(seed), 8)
    queries = draw_queries(jax.random.fold_in(streams_of[7], 71), 0)
    visual_keys = draw_visual_keys(jax.random.fold_in(streams_of[7], 71), 0)
    visual_values = scatter_about(streams_of[2], (LAYERS, KEYS, D), 1.0, 6.0, ((1, 4),))
    out_grad = scatter_about(streams_of[3], (LAYERS, TOKENS, D), 1.0, 6.0, ((1, 64), (2, 4)))
    gate_value = jnp.clip(jax.random.uniform(streams_of[4], (LAYERS, H), jnp.float32, -1.5, 1.5) * shard_levels(streams_of[4], (LAYERS, H), ((1, 4),), -0.4, 0.0), -1.5, 1.5)
    image_order = draw_image_order(jax.random.fold_in(streams_of[7], 71), 0)
    image_seen = set_ends(jax.random.randint(streams_of[6], (TOKENS,), 1, IMAGES + 1), jax.random.fold_in(streams_of[6], 1), 1, IMAGES).astype(jnp.int32)
    return dict(queries=queries, visual_keys=visual_keys, visual_values=visual_values, out_grad=out_grad, gate_value=gate_value, image_order=image_order, image_seen=image_seen)


def rounded(array):
    return lax.optimization_barrier(array.astype(jnp.bfloat16)).astype(jnp.float32)

def reference(queries, visual_keys, visual_values, out_grad, gate_value, image_order, image_seen):
    score_scale = 1.0 / math.sqrt(HD)
    block_count = TOKENS // TOK_DEV
    query_list = []
    key_list = []
    value_list = []
    for layer_index in range(LAYERS):
        key_image = jnp.broadcast_to(image_order[layer_index][:, None], (IMAGES, LAT)).reshape(KEYS)
        key_heads = visual_keys[layer_index].astype(jnp.float32).reshape(KEYS, H, HD)
        value_heads = visual_values[layer_index].astype(jnp.float32).reshape(KEYS, H, HD)
        factor = jnp.tanh(gate_value[layer_index])

        def block_step(totals, pieces):
            query_block, grad_block, seen_block = pieces
            query_heads = query_block.astype(jnp.float32).reshape(TOK_DEV, H, HD)
            gated_grad = rounded(grad_block.astype(jnp.float32).reshape(TOK_DEV, H, HD) * factor[None, :, None])
            allowed = key_image[None, :] < seen_block[:, None]
            scores = jnp.einsum('thd,khd->htk', query_heads, key_heads) * score_scale
            masked = jnp.where(allowed[None], scores, -1e+30)
            row_max = lax.optimization_barrier(jnp.max(masked, axis=2, keepdims=True))
            exponent = jnp.where(allowed[None], jnp.exp(masked - row_max), 0.0)
            weights = exponent / lax.optimization_barrier(jnp.sum(exponent, axis=2, keepdims=True))
            weight_half = rounded(weights)
            attended = jnp.einsum('htk,khd->thd', weight_half, value_heads)
            row_delta = lax.optimization_barrier(jnp.sum(gated_grad * attended, axis=2))
            weight_grad = jnp.einsum('thd,khd->htk', gated_grad, value_heads)
            score_half = rounded(weights * (weight_grad - jnp.transpose(row_delta)[:, :, None]))
            query_part = (jnp.einsum('htk,khd->thd', score_half, key_heads) * score_scale).astype(jnp.bfloat16)
            key_part = jnp.einsum('htk,thd->khd', score_half, query_heads) * score_scale
            value_part = jnp.einsum('htk,thd->khd', weight_half, gated_grad)
            new_totals = (totals[0] + key_part.reshape(KEYS, D), totals[1] + value_part.reshape(KEYS, D))
            return (new_totals, query_part.reshape(TOK_DEV, D))
        inputs = (queries[layer_index].reshape(block_count, TOK_DEV, D), out_grad[layer_index].reshape(block_count, TOK_DEV, D), image_seen.reshape(block_count, TOK_DEV))
        empty_sum = jnp.zeros((KEYS, D), jnp.float32)
        sums, query_parts = lax.scan(block_step, (empty_sum, empty_sum), inputs)
        query_list.append(query_parts.reshape(TOKENS, D))
        key_list.append(sums[0])
        value_list.append(sums[1])
    return (jnp.stack(query_list), jnp.stack(key_list), jnp.stack(value_list))
```

```python
import functools
import math

import jax
import jax.numpy as jnp
from jax import lax
from jax.experimental import pallas as pl
from jax.experimental.pallas import tpu as pltpu
from jax.sharding import Mesh, PartitionSpec as P

HEAD = 128
NT = (((1,), (1,)), ((), ()))
NN = (((1,), (0,)), ((), ()))
TN = (((0,), (0,)), ((), ()))
LOG2E = math.log2(math.e)
CHUNKS = 1
AXES = ("yh", "c", "x", "yl", "z")


def head_grads(query, grad_in, keys, values, factor, allowed, scale):
    gated = (grad_in.astype(jnp.float32) * factor).astype(jnp.bfloat16)
    block = keys.shape[0] // len(allowed)
    scores = lax.dot_general(keys, query, NT, preferred_element_type=jnp.float32)
    scores = jnp.concatenate(
        [jnp.where(a, scores[b * block : (b + 1) * block], -1e30) for b, a in enumerate(allowed)], axis=0
    )
    top = jnp.max(scores, axis=0, keepdims=True)
    exponent = jnp.exp2((scores - top) * (scale * LOG2E))
    weights = exponent * (1.0 / jnp.sum(exponent, axis=0, keepdims=True))
    weights_half = weights.astype(jnp.bfloat16)
    weight_grad = lax.dot_general(values, gated, NT, preferred_element_type=jnp.float32)
    row_delta = jnp.sum(weights_half.astype(jnp.float32) * weight_grad, axis=0, keepdims=True)
    score_half = (weights * (weight_grad - row_delta)).astype(jnp.bfloat16)
    query_part = lax.dot_general(keys, score_half, TN, preferred_element_type=jnp.float32) * scale
    key_part = lax.dot_general(score_half, query, NN, preferred_element_type=jnp.float32) * scale
    value_part = lax.dot_general(weights_half, gated, NN, preferred_element_type=jnp.float32)
    return jnp.transpose(query_part), key_part, value_part


def attention_body(
    place, order, factor, seen, query, grad_in, key_own, value_own, key_pair, value_pair,
    unit_0, unit_1, unit_2, unit_3, *rest, first, scale,
):
    query_out, key_send, key_keep, value_send, value_keep, latents, key_rows, value_rows = rest[-8:]
    head = first + pl.program_id(0)
    sources = (key_own, value_own, key_pair, value_pair, unit_0, unit_1, unit_2, unit_3)
    for i, source in enumerate(sources):
        latents[pl.ds(pl.multiple_of(place[1 + i], 128), 128), :] = source[...].reshape(128, HEAD)
    allowed = [order[b] < seen[...] for b in range(8)]
    total = latents.shape[0] // 2
    query_part, key_part, value_part = head_grads(
        query[...], grad_in[...], latents[:total], latents[total:], factor[head], allowed, scale
    )
    query_out[...] = query_part.astype(jnp.bfloat16)
    key_rows[...] = key_part.astype(jnp.bfloat16)
    value_rows[...] = value_part.astype(jnp.bfloat16)
    for rows, outs, at in ((key_rows, (key_send, key_keep), 9), (value_rows, (value_send, value_keep), 13)):
        for i in range(4):
            outs[i // 2][pl.ds(i % 2 * 128, 128), :] = rows[pl.ds(pl.multiple_of(place[at + i], 128), 128), :]


def attention(place, order, factor, seen, query, grad_in, key_own, value_own, pair, units, buffer, first, count):
    tokens = query.shape[0]
    scalar = pl.BlockSpec(memory_space=pltpu.SMEM)
    head_of = lambda h, place: (0, first + h)
    own_of = lambda h, place: (0, place[0] + first + h)
    part = lambda rows: pl.BlockSpec((rows, HEAD), lambda h, place: (0, h))
    grads = jax.ShapeDtypeStruct((256, count * HEAD), jnp.bfloat16)
    grid_spec = pltpu.PrefetchScalarGridSpec(
        num_scalar_prefetch=1,
        grid=(count,),
        in_specs=[
            scalar,
            scalar,
            pl.BlockSpec((1, tokens), lambda h, place: (0, 0)),
            pl.BlockSpec((tokens, HEAD), head_of),
            pl.BlockSpec((tokens, HEAD), head_of),
            pl.BlockSpec((128, HEAD), own_of),
            pl.BlockSpec((128, HEAD), own_of),
            pl.BlockSpec((1, 128, HEAD), lambda h, place: (0, 0, h)),
            pl.BlockSpec((1, 128, HEAD), lambda h, place: (1, 0, h)),
            part(128),
            part(128),
            part(128),
            part(128),
        ] + [pl.BlockSpec(memory_space=pl.ANY)] * len(buffer),
        out_specs=[pl.BlockSpec((tokens, HEAD), head_of)] + [part(256)] * 4,
        scratch_shapes=[
            pltpu.VMEM((1024, HEAD), jnp.bfloat16),
            pltpu.VMEM((512, HEAD), jnp.bfloat16),
            pltpu.VMEM((512, HEAD), jnp.bfloat16),
        ],
    )
    matmul = 2 * tokens * 512 * HEAD
    return pl.pallas_call(
        functools.partial(attention_body, first=first, scale=1.0 / math.sqrt(HEAD)),
        grid_spec=grid_spec,
        out_shape=[jax.ShapeDtypeStruct(query.shape, jnp.bfloat16)] + [grads] * 4,
        input_output_aliases={14: 0} if buffer else {},
        compiler_params=pltpu.CompilerParams(
            dimension_semantics=("arbitrary",), vmem_limit_bytes=48 * 2**20
        ),
        cost_estimate=pl.CostEstimate(
            flops=5 * count * matmul, transcendentals=count * tokens * 512, bytes_accessed=count * 2**20
        ),
        name="attention",
    )(place, order, factor, seen, query, grad_in, key_own, value_own, pair, pair, *units, *buffer)


def relabel(sizes, move):
    pairs = []
    total = math.prod(sizes)
    for source in range(total):
        rest, at = source, []
        for size in reversed(sizes):
            at.append(rest % size)
            rest //= size
        to = 0
        for index, size in zip(move(*reversed(at)), sizes):
            to = to * size + index % size
        pairs.append((source, to))
    return pairs


def columns(array, start, width):
    return lax.dynamic_slice(array, (0, start), (array.shape[0], width))


def shards(queries, visual_keys, visual_values, out_grad, gate_value, image_order, image_seen):
    query, grad_in, keys, values = queries[0], out_grad[0], visual_keys[0], visual_values[0]
    local = query.shape[1]
    heads = local // HEAD
    yh, c, x, yl, z = (lax.axis_index(a) for a in AXES)
    colour = lambda x, z, c: (x + 2 * z) % 4 ^ c
    row_block = lambda owner: owner * 128
    unit_at = lambda unit: unit // 2 * 512 + row_block((1 - yh) * 2 + unit % 2)
    own = yh * 2 + c
    pair_owner = yh * 2 + 1 - c
    place = [own * heads, row_block(own), 512 + row_block(own), row_block(pair_owner), 512 + row_block(pair_owner)]
    place += [unit_at(colour(x + dx, z + dz, c)) for dx, dz in ((0, 0), (3, 0), (1, 0), (0, 7))]
    step = x ^ 1
    cross = 3 - x
    place += [row_block(b) for b in (3 - step, step, cross, x)]
    place += [row_block(b) for b in (cross ^ 1, cross, step, x)]
    place = jnp.stack(place).astype(jnp.int32)
    factor = jnp.tanh(gate_value[0])
    seen = image_seen[None]

    to_cross = relabel((2, 2, 4, 2), lambda yh, c, x, yl: (1 - yh, c ^ (x & 1), x, 1 - yl))
    flip_pairs = [(i, i ^ 1) for i in range(4)]
    cross_pairs = [(i, 3 - i) for i in range(4)]
    there = (1 - yh) * 2 + (c ^ (x & 1))
    wants_values = (x + 2 * z) % 4 // 2 == 1

    count = heads // CHUNKS
    width = count * HEAD
    gathered = []
    for n in range(CHUNKS):
        at = n * width
        pair = jnp.stack([columns(a, pair_owner * local + at, width) for a in (keys, values)])
        pair = lax.ppermute(pair, "c", [(0, 1), (1, 0)])
        sent = jnp.where(
            wants_values, columns(values, there * local + at, width), columns(keys, there * local + at, width)
        )
        unit = lax.ppermute(sent, ("yh", "c", "x", "yl"), to_cross)
        units = [
            unit,
            lax.ppermute(unit, "x", [(i, (i + 1) % 4) for i in range(4)]),
            lax.ppermute(unit, "x", [(i, (i + 3) % 4) for i in range(4)]),
            lax.ppermute(unit, "z", [(i, (i + 1) % 8) for i in range(8)]),
        ]
        gathered.append((pair, units))

    query_grad = ()
    parts = []
    f32 = jnp.float32
    for n in range(CHUNKS):
        pair, units = gathered[n]
        whole, key_send, key_keep, value_send, value_keep = attention(
            place, image_order[0], factor, seen, query, grad_in, keys, values, pair, units,
            query_grad, n * count, count,
        )
        query_grad = (whole,)
        mine = []
        for send, keep, first, second in (
            (key_send, key_keep, flip_pairs, cross_pairs),
            (value_send, value_keep, cross_pairs, flip_pairs),
        ):
            got = lax.ppermute(send, "x", first)
            passed = (keep[:128].astype(f32) + got[:128].astype(f32)).astype(jnp.bfloat16)
            passed = lax.ppermute(passed, "x", second)
            mine.append(
                (keep[128:].astype(f32) + got[128:].astype(f32) + passed.astype(f32)).astype(jnp.bfloat16)
            )
        both = jnp.stack([m.reshape(16, 8, width) for m in mine], axis=1)
        arrived = lax.all_to_all(both, ("yl", "z"), split_axis=0, concat_axis=0, tiled=True)
        parts.append(arrived.astype(f32).sum(axis=0))
    result = jnp.concatenate(parts, axis=2)
    return whole[None], result[0][None], result[1][None]


def solution(mesh):
    torus = Mesh(mesh.devices.reshape(2, 2, 4, 2, 8), AXES)
    img, txt = ("yh", "c"), ("x", "yl", "z")
    placed = (
        P(None, txt, img),
        P(None, img, None),
        P(None, img, None),
        P(None, txt, img),
        P(None, img),
        P(),
        P(txt),
    )
    return jax.shard_map(
        shards, mesh=torus, in_specs=placed, out_specs=(P(None, txt, img),) * 3, check_vma=False
    )
```

```python
import functools
import math

import jax
import jax.numpy as jnp
from jax import lax
from jax.experimental import pallas as pl
from jax.experimental.pallas import tpu as pltpu
from jax.sharding import Mesh, PartitionSpec as P


HEAD = 128
NT = (((1,), (1,)), ((), ()))
NN = (((1,), (0,)), ((), ()))
TN = (((0,), (0,)), ((), ()))
LOG2E = math.log2(math.e)
GATHERS = ((6,), (4, 3, 3))
PLANES = ((0,), (1, 2, 3))
AXES = ("yh", "c", "x", "yl", "z")


def head_grads(query, grad_in, keys, values, factor, allowed, scale):
    gated = (grad_in.astype(jnp.float32) * factor).astype(jnp.bfloat16)
    block = keys.shape[0] // len(allowed)
    scores = lax.dot_general(keys, query, NT, preferred_element_type=jnp.float32)
    scores = jnp.concatenate(
        [jnp.where(a, scores[b * block : (b + 1) * block], -1e30) for b, a in enumerate(allowed)], axis=0
    )
    top = jnp.max(scores, axis=0, keepdims=True)
    exponent = jnp.exp2((scores - top) * (scale * LOG2E))
    weights = exponent * (1.0 / jnp.sum(exponent, axis=0, keepdims=True))
    weights_half = weights.astype(jnp.bfloat16)
    weight_grad = lax.dot_general(values, gated, NT, preferred_element_type=jnp.float32)
    row_delta = jnp.sum(weights_half.astype(jnp.float32) * weight_grad, axis=0, keepdims=True)
    score_half = (weights * (weight_grad - row_delta)).astype(jnp.bfloat16)
    query_part = lax.dot_general(keys, score_half, TN, preferred_element_type=jnp.float32) * scale
    key_part = lax.dot_general(score_half, query, NN, preferred_element_type=jnp.float32) * scale
    value_part = lax.dot_general(weights_half, gated, NN, preferred_element_type=jnp.float32)
    return jnp.transpose(query_part), key_part, value_part


def attention_body(
    place, order, factor, seen, query, grad_in, key_own, value_own, key_pair, value_pair,
    unit_0, unit_1, unit_2, unit_3, *rest, first, scale,
):
    query_out, key_send, key_keep, value_send, value_keep, latents, key_rows, value_rows = rest[-8:]
    head = first + pl.program_id(0)
    sources = (key_own, value_own, key_pair, value_pair, unit_0, unit_1, unit_2, unit_3)
    for i, source in enumerate(sources):
        latents[pl.ds(pl.multiple_of(place[1 + i], 128), 128), :] = source[...].reshape(128, HEAD)
    allowed = [order[b] < seen[...] for b in range(8)]
    total = latents.shape[0] // 2
    query_part, key_part, value_part = head_grads(
        query[...], grad_in[...], latents[:total], latents[total:], factor[head], allowed, scale
    )
    query_out[...] = query_part.astype(jnp.bfloat16)
    key_rows[...] = key_part.astype(jnp.bfloat16)
    value_rows[...] = value_part.astype(jnp.bfloat16)
    for rows, outs, at in ((key_rows, (key_send, key_keep), 9), (value_rows, (value_send, value_keep), 13)):
        for i in range(4):
            outs[i // 2][pl.ds(i % 2 * 128, 128), :] = rows[pl.ds(pl.multiple_of(place[at + i], 128), 128), :]


def attention(place, order, factor, seen, query, grad_in, key_own, value_own, pair, units, buffer, first, count, offset):
    tokens = query.shape[0]
    scalar = pl.BlockSpec(memory_space=pltpu.SMEM)
    head_of = lambda h, place: (0, first + h)
    own_of = lambda h, place: (0, place[0] + first + h)
    part = lambda rows, at=0: pl.BlockSpec((rows, HEAD), lambda h, place: (0, at + h))
    grads = jax.ShapeDtypeStruct((256, count * HEAD), jnp.bfloat16)
    grid_spec = pltpu.PrefetchScalarGridSpec(
        num_scalar_prefetch=1,
        grid=(count,),
        in_specs=[
            scalar,
            scalar,
            pl.BlockSpec((1, tokens), lambda h, place: (0, 0)),
            pl.BlockSpec((tokens, HEAD), head_of),
            pl.BlockSpec((tokens, HEAD), head_of),
            pl.BlockSpec((128, HEAD), own_of),
            pl.BlockSpec((128, HEAD), own_of),
            pl.BlockSpec((1, 128, HEAD), lambda h, place: (0, 0, offset + h)),
            pl.BlockSpec((1, 128, HEAD), lambda h, place: (1, 0, offset + h)),
            part(128, offset),
            part(128, offset),
            part(128, offset),
            part(128, offset),
        ] + [pl.BlockSpec(memory_space=pl.ANY)] * len(buffer),
        out_specs=[pl.BlockSpec((tokens, HEAD), head_of)] + [part(256)] * 4,
        scratch_shapes=[
            pltpu.VMEM((1024, HEAD), jnp.bfloat16),
            pltpu.VMEM((512, HEAD), jnp.bfloat16),
            pltpu.VMEM((512, HEAD), jnp.bfloat16),
        ],
    )
    matmul = 2 * tokens * 512 * HEAD
    return pl.pallas_call(
        functools.partial(attention_body, first=first, scale=1.0 / math.sqrt(HEAD)),
        grid_spec=grid_spec,
        out_shape=[jax.ShapeDtypeStruct(query.shape, jnp.bfloat16)] + [grads] * 4,
        input_output_aliases={14: 0} if buffer else {},
        compiler_params=pltpu.CompilerParams(
            dimension_semantics=("arbitrary",), vmem_limit_bytes=48 * 2**20
        ),
        cost_estimate=pl.CostEstimate(
            flops=5 * count * matmul, transcendentals=count * tokens * 512, bytes_accessed=count * 2**20
        ),
        name="attention",
    )(place, order, factor, seen, query, grad_in, key_own, value_own, pair, pair, *units, *buffer)


def relabel(sizes, move):
    pairs = []
    total = math.prod(sizes)
    for source in range(total):
        rest, at = source, []
        for size in reversed(sizes):
            at.append(rest % size)
            rest //= size
        to = 0
        for index, size in zip(move(*reversed(at)), sizes):
            to = to * size + index % size
        pairs.append((source, to))
    return pairs


def columns(array, start, width):
    return lax.dynamic_slice(array, (0, start), (array.shape[0], width))


def shards(queries, visual_keys, visual_values, out_grad, gate_value, image_order, image_seen):
    query, grad_in, keys, values = queries[0], out_grad[0], visual_keys[0], visual_values[0]
    local = query.shape[1]
    heads = local // HEAD
    yh, c, x, _, z = (lax.axis_index(a) for a in AXES)
    colour = lambda x, z, c: (x + 2 * z) % 4 ^ c
    row_block = lambda owner: owner * 128
    unit_at = lambda unit: unit // 2 * 512 + row_block((1 - yh) * 2 + unit % 2)
    own = yh * 2 + c
    pair_owner = yh * 2 + 1 - c
    place = [own * heads, row_block(own), 512 + row_block(own), row_block(pair_owner), 512 + row_block(pair_owner)]
    place += [unit_at(colour(x + dx, z + dz, c)) for dx, dz in ((0, 0), (3, 0), (1, 0), (0, 7))]
    step = x ^ 1
    cross = 3 - x
    place += [row_block(b) for b in (3 - step, step, cross, x)]
    place += [row_block(b) for b in (cross ^ 1, cross, step, x)]
    place = jnp.stack(place).astype(jnp.int32)
    factor = jnp.tanh(gate_value[0])
    seen = image_seen[None]

    to_cross = relabel((2, 2, 4, 2), lambda yh, c, x, yl: (1 - yh, c ^ (x & 1), x, 1 - yl))
    flip_pairs = [(i, i ^ 1) for i in range(4)]
    cross_pairs = [(i, 3 - i) for i in range(4)]
    there = (1 - yh) * 2 + (c ^ (x & 1))
    wants_values = (x + 2 * z) % 4 // 2 == 1

    gathered = []
    first = 0
    for counts in GATHERS:
        at, width = first * HEAD, sum(counts) * HEAD
        sent = jnp.where(
            wants_values, columns(values, there * local + at, width), columns(keys, there * local + at, width)
        )
        pair = jnp.stack([columns(a, pair_owner * local + at, width) for a in (keys, values)])
        unit = lax.ppermute(sent, ("yh", "c", "x", "yl"), to_cross)
        pair = lax.ppermute(pair, "c", [(0, 1), (1, 0)])
        units = [unit]
        for axis, size, by in (("x", 4, 1), ("x", 4, 3), ("z", 8, 1)):
            units.append(lax.ppermute(unit, axis, [(i, (i + by) % size) for i in range(size)]))
        offset = 0
        for count in counts:
            gathered.append((pair, units, first, count, offset))
            first += count
            offset += count

    buffer = ()
    ready, parts = [], []
    f32 = jnp.float32
    for pair, units, first, count, offset in gathered:
        whole, key_send, key_keep, value_send, value_keep = attention(
            place, image_order[0], factor, seen, query, grad_in, keys, values, pair, units,
            buffer, first, count, offset,
        )
        buffer = (whole,)
        mine = []
        for send, keep, near, far in (
            (key_send, key_keep, flip_pairs, cross_pairs), (value_send, value_keep, cross_pairs, flip_pairs)
        ):
            got = lax.ppermute(send, "x", near)
            passed = (keep[:128].astype(f32) + got[:128].astype(f32)).astype(jnp.bfloat16)
            passed = lax.ppermute(passed, "x", far)
            mine.append(
                (keep[128:].astype(f32) + got[128:].astype(f32) + passed.astype(f32)).astype(jnp.bfloat16)
            )
        ready.append(jnp.stack([m.reshape(16, 8, count * HEAD) for m in mine], axis=1))
    for members in PLANES:
        both = jnp.concatenate([ready[m] for m in members], axis=3)
        arrived = lax.all_to_all(both, ("yl", "z"), split_axis=0, concat_axis=0, tiled=True)
        parts.append(arrived.astype(f32).sum(axis=0))
    result = jnp.concatenate(parts, axis=2)
    return whole[None], result[0][None], result[1][None]


def solution(mesh):
    torus = Mesh(mesh.devices.reshape(2, 2, 4, 2, 8), AXES)
    img, txt = ("yh", "c"), ("x", "yl", "z")
    placed = (
        P(None, txt, img),
        P(None, img, None),
        P(None, img, None),
        P(None, txt, img),
        P(None, img),
        P(),
        P(txt),
    )
    return jax.shard_map(shards, mesh=torus, in_specs=placed, out_specs=(P(None, txt, img),) * 3, check_vma=False)
```

```python
import functools
import math

import jax
import jax.numpy as jnp
from jax import lax
from jax.experimental import pallas as pl
from jax.experimental.pallas import tpu as pltpu
from jax.sharding import Mesh, PartitionSpec as P


HEAD = 128
NT = (((1,), (1,)), ((), ()))
NN = (((1,), (0,)), ((), ()))
TN = (((0,), (0,)), ((), ()))
LOG2E = math.log2(math.e)
SCALE = 1.0 / math.sqrt(HEAD)
GATHERS = ((8,), (8,))
PLANES = ((0,), (1,))
AXES = ("yh", "c", "x", "yl", "z")


def score_stage(query, grad_in, keys, values, factor):
    gated = (grad_in.astype(jnp.float32) * factor).astype(jnp.bfloat16)
    scores = lax.dot_general(keys, query, NT, preferred_element_type=jnp.float32)
    weight_grad = lax.dot_general(values, gated, NT, preferred_element_type=jnp.float32)
    return scores, weight_grad, gated


def by_eights(op, blocks):
    folded = [op(b.reshape(-1, 8, b.shape[1]), axis=0) for b in blocks]
    return functools.reduce(jnp.maximum if op is jnp.max else jnp.add, folded)


def weight_stage(scores, weight_grad, allowed, scale):
    block = scores.shape[0] // len(allowed)
    cut = lambda array: [array[b * block : (b + 1) * block] for b in range(len(allowed))]
    masked = [jnp.where(a, s, -1e30) for a, s in zip(allowed, cut(scores))]
    grads = cut(weight_grad)
    top = jnp.max(by_eights(jnp.max, masked), axis=0, keepdims=True)
    exponent = [jnp.exp2((m - top) * (scale * LOG2E)) for m in masked]
    share = 1.0 / jnp.sum(by_eights(jnp.sum, exponent), axis=0, keepdims=True)
    crossed = by_eights(jnp.sum, [e * g for e, g in zip(exponent, grads)])
    row_delta = jnp.sum(crossed, axis=0, keepdims=True) * share
    weights = [e * share for e in exponent]
    weights_half = jnp.concatenate([w.astype(jnp.bfloat16) for w in weights], axis=0)
    score_half = jnp.concatenate(
        [(w * (g - row_delta)).astype(jnp.bfloat16) for w, g in zip(weights, grads)], axis=0
    )
    return weights_half, score_half


def attention_body(
    place, order, factor, seen, query, grad_in, key_own, value_own, key_pair, value_pair,
    unit_0, unit_1, unit_2, unit_3, *rest, first, scale, step,
):
    query_out, key_send, key_keep, value_send, value_keep, latents = rest[-6:]
    head = first + pl.program_id(0) * step
    sources = (key_own, value_own, key_pair, value_pair, unit_0, unit_1, unit_2, unit_3)
    for i, source in enumerate(sources):
        latents[pl.ds(pl.multiple_of(place[1 + i], 128), 128), :] = source[...].reshape(128, step * HEAD)
    allowed = [order[place[9 + b]] < seen[...] for b in range(8)]
    total = latents.shape[0] // 2
    at = [slice(i * HEAD, (i + 1) * HEAD) for i in range(step)]
    scored, weighed = [None] * step, [None] * step

    def score(i):
        scored[i] = score_stage(
            query[:, at[i]], grad_in[:, at[i]], latents[:total, at[i]], latents[total:, at[i]], factor[head + i]
        )

    def weigh(i):
        weighed[i] = weight_stage(scored[i][0], scored[i][1], allowed, scale)

    def project(i):
        weights_half, score_half = weighed[i]
        dot = lambda a, b, dims: lax.dot_general(a, b, dims, preferred_element_type=jnp.float32)
        query_part = dot(latents[:total, at[i]], score_half, TN) * scale
        query_out[:, at[i]] = jnp.transpose(query_part).astype(jnp.bfloat16)
        key_part = dot(score_half, query[:, at[i]], NN).astype(jnp.bfloat16)
        key_send[:, at[i]] = key_part[:256]
        key_keep[:, at[i]] = key_part[256:]
        value_part = dot(weights_half, scored[i][2], NN).astype(jnp.bfloat16)
        for slot, (out, row) in enumerate(((value_send, 0), (value_keep, 0), (value_send, 128), (value_keep, 128))):
            out[row : row + 128, at[i]] = value_part[slot * 128 : (slot + 1) * 128]

    score(0)
    for i in range(step):
        if i + 1 < step:
            score(i + 1)
        weigh(i)
        if i:
            project(i - 1)
    project(step - 1)


def attention(place, order, factor, seen, query, grad_in, key_own, value_own, pair, units, buffer, first, count, offset):
    tokens = query.shape[0]
    step = next(s for s in (4, 3, 2, 1) if count % s == first % s == offset % s == 0)
    width = step * HEAD
    scalar = pl.BlockSpec(memory_space=pltpu.SMEM)
    head_of = lambda h, place: (0, first // step + h)
    own_of = lambda h, place: (0, place[0] // step + first // step + h)
    part = lambda rows, at=0: pl.BlockSpec((rows, width), lambda h, place: (0, at // step + h))
    paired = lambda which: pl.BlockSpec((1, 128, width), lambda h, place: (which, 0, offset // step + h))
    grads = jax.ShapeDtypeStruct((256, count * HEAD), jnp.bfloat16)
    grid_spec = pltpu.PrefetchScalarGridSpec(
        num_scalar_prefetch=1,
        grid=(count // step,),
        in_specs=[
            scalar,
            scalar,
            pl.BlockSpec((1, tokens), lambda h, place: (0, 0)),
            pl.BlockSpec((tokens, width), head_of),
            pl.BlockSpec((tokens, width), head_of),
            pl.BlockSpec((128, width), own_of),
            pl.BlockSpec((128, width), own_of),
            paired(0),
            paired(1),
        ]
        + [part(128, offset)] * 4
        + [pl.BlockSpec(memory_space=pl.ANY)] * len(buffer),
        out_specs=[pl.BlockSpec((tokens, width), head_of)] + [part(256)] * 4,
        scratch_shapes=[pltpu.VMEM((1024, width), jnp.bfloat16)],
    )
    matmul = 2 * tokens * 512 * HEAD
    return pl.pallas_call(
        functools.partial(attention_body, first=first, scale=SCALE, step=step),
        grid_spec=grid_spec,
        out_shape=[jax.ShapeDtypeStruct(query.shape, jnp.bfloat16)] + [grads] * 4,
        input_output_aliases={14: 0} if buffer else {},
        compiler_params=pltpu.CompilerParams(dimension_semantics=("arbitrary",), vmem_limit_bytes=48 * 2**20),
        cost_estimate=pl.CostEstimate(
            flops=5 * count * matmul, transcendentals=count * tokens * 512, bytes_accessed=count * 2**20
        ),
        name="attention",
    )(place, order, factor, seen, query, grad_in, key_own, value_own, pair, pair, *units, *buffer)


def relabel(sizes, move):
    pairs = []
    total = math.prod(sizes)
    for source in range(total):
        rest, at = source, []
        for size in reversed(sizes):
            at.append(rest % size)
            rest //= size
        to = 0
        for index, size in zip(move(*reversed(at)), sizes):
            to = to * size + index % size
        pairs.append((source, to))
    return pairs


def columns(array, start, width):
    return lax.dynamic_slice(array, (0, start), (array.shape[0], width))


def shards(queries, visual_keys, visual_values, out_grad, gate_value, image_order, image_seen):
    query, grad_in, keys, values = queries[0], out_grad[0], visual_keys[0], visual_values[0]
    local = query.shape[1]
    heads = local // HEAD
    yh, c, x, _, z = (lax.axis_index(a) for a in AXES)
    colour = lambda x, z, c: (x + 2 * z) % 4 ^ c
    slot = lambda owner: 135 >> 2 * (owner ^ x) & 3
    row_block = lambda owner: slot(owner) * 128
    unit_at = lambda unit: unit // 2 * 512 + row_block((1 - yh) * 2 + unit % 2)
    own = yh * 2 + c
    pair_owner = yh * 2 + 1 - c
    place = [own * heads, row_block(own), 512 + row_block(own), row_block(pair_owner), 512 + row_block(pair_owner)]
    place += [unit_at(colour(x + dx, z + dz, c)) for dx, dz in ((0, 0), (3, 0), (1, 0), (0, 7))]
    place += [(x ^ flip) * 2 + half for flip in (2, 1, 3, 0) for half in (0, 1)]
    place = jnp.stack(place).astype(jnp.int32)
    factor = jnp.tanh(gate_value[0])
    seen = image_seen[None]

    to_cross = relabel((2, 2, 4, 2), lambda yh, c, x, yl: (1 - yh, c ^ (x & 1), x, 1 - yl))
    flip_pairs = [(i, i ^ 1) for i in range(4)]
    cross_pairs = [(i, 3 - i) for i in range(4)]
    there = (1 - yh) * 2 + (c ^ (x & 1))
    wants_values = (x + 2 * z) % 4 // 2 == 1

    gathered = []
    first = 0
    for counts in GATHERS:
        at, width = first * HEAD, sum(counts) * HEAD
        sent = jnp.where(
            wants_values, columns(values, there * local + at, width), columns(keys, there * local + at, width)
        )
        pair = jnp.stack([columns(a, pair_owner * local + at, width) for a in (keys, values)])
        unit = lax.ppermute(sent, ("yh", "c", "x", "yl"), to_cross)
        pair = lax.ppermute(pair, "c", [(0, 1), (1, 0)])
        units = [unit]
        for axis, size, by in (("x", 4, 1), ("x", 4, 3), ("z", 8, 1)):
            units.append(lax.ppermute(unit, axis, [(i, (i + by) % size) for i in range(size)]))
        offset = 0
        for count in counts:
            gathered.append((pair, units, first, count, offset))
            first += count
            offset += count

    buffer = ()
    ready, parts = [], []
    f32 = jnp.float32
    for pair, units, first, count, offset in gathered:
        whole, key_send, key_keep, value_send, value_keep = attention(
            place, image_order[0], factor, seen, query, grad_in, keys, values, pair, units,
            buffer, first, count, offset,
        )
        buffer = (whole,)
        mine = []
        for send, keep, near, far in (
            (key_send, key_keep, flip_pairs, cross_pairs), (value_send, value_keep, cross_pairs, flip_pairs)
        ):
            got = lax.ppermute(send, "x", near)
            passed = (keep[:128].astype(f32) + got[:128].astype(f32)).astype(jnp.bfloat16)
            passed = lax.ppermute(passed, "x", far)
            mine.append(
                (keep[128:].astype(f32) + got[128:].astype(f32) + passed.astype(f32)).astype(jnp.bfloat16)
            )
        ready.append(jnp.stack([m.reshape(16, 8, count * HEAD) for m in mine], axis=1))
    for members in PLANES:
        both = jnp.concatenate([ready[m] for m in members], axis=3)
        arrived = lax.all_to_all(both, ("yl", "z"), split_axis=0, concat_axis=0, tiled=True)
        parts.append(arrived.astype(f32).sum(axis=0))
    result = jnp.concatenate(parts, axis=2)
    return whole[None], result[0][None] * SCALE, result[1][None]


def solution(mesh):
    torus = Mesh(mesh.devices.reshape(2, 2, 4, 2, 8), AXES)
    img, txt = ("yh", "c"), ("x", "yl", "z")
    placed = (
        P(None, txt, img),
        P(None, img, None),
        P(None, img, None),
        P(None, txt, img),
        P(None, img),
        P(),
        P(txt),
    )
    return jax.shard_map(shards, mesh=torus, in_specs=placed, out_specs=(P(None, txt, img),) * 3, check_vma=False)
```

```python
import functools
import math

import jax
import jax.numpy as jnp
from jax import lax
from jax.experimental import pallas as pl
from jax.experimental.pallas import tpu as pltpu
from jax.sharding import Mesh, PartitionSpec as P


HEAD = 128
NT = (((1,), (1,)), ((), ()))
NN = (((1,), (0,)), ((), ()))
TN = (((0,), (0,)), ((), ()))
LOG2E = math.log2(math.e)
SCALE = 1.0 / math.sqrt(HEAD)
GATHERS = ((8,), (8,))
PLANES = ((0,), (1,))
AXES = ("yh", "c", "x", "yl", "z")


def score_stage(query, grad_in, keys, values, factor):
    gated = (grad_in.astype(jnp.float32) * factor).astype(jnp.bfloat16)
    scores = lax.dot_general(keys, query, NT, preferred_element_type=jnp.float32)
    weight_grad = lax.dot_general(values, gated, NT, preferred_element_type=jnp.float32)
    return scores, weight_grad, gated


def by_eights(op, blocks):
    folded = [op(b.reshape(-1, 8, b.shape[1]), axis=0) for b in blocks]
    return functools.reduce(jnp.maximum if op is jnp.max else jnp.add, folded)


def weight_stage(scores, weight_grad, allowed, scale):
    block = scores.shape[0] // len(allowed)
    cut = lambda array: [array[b * block : (b + 1) * block] for b in range(len(allowed))]
    masked = [jnp.where(a, s, -1e30) for a, s in zip(allowed, cut(scores))]
    grads = cut(weight_grad)
    top = jnp.max(by_eights(jnp.max, masked), axis=0, keepdims=True)
    exponent = [jnp.exp2((m - top) * (scale * LOG2E)) for m in masked]
    share = 1.0 / jnp.sum(by_eights(jnp.sum, exponent), axis=0, keepdims=True)
    crossed = by_eights(jnp.sum, [e * g for e, g in zip(exponent, grads)])
    row_delta = jnp.sum(crossed, axis=0, keepdims=True) * share
    weights = [e * share for e in exponent]
    weights_half = jnp.concatenate([w.astype(jnp.bfloat16) for w in weights], axis=0)
    score_half = jnp.concatenate(
        [(w * (g - row_delta)).astype(jnp.bfloat16) for w, g in zip(weights, grads)], axis=0
    )
    return weights_half, score_half


def attention_body(
    place, order, factor, seen, query, grad_in, key_own, value_own, key_pair, value_pair,
    unit_0, unit_1, unit_2, unit_3, *rest, first, scale, step,
):
    query_out, key_send, key_keep, value_send, value_keep, latents = rest[-6:]
    head = first + pl.program_id(0) * step
    sources = (key_own, value_own, key_pair, value_pair, unit_0, unit_1, unit_2, unit_3)
    for i, source in enumerate(sources):
        latents[pl.ds(pl.multiple_of(place[1 + i], 128), 128), :] = source[...].reshape(128, step * HEAD)
    allowed = [order[place[9 + b]] < seen[...] for b in range(8)]
    total = latents.shape[0] // 2
    at = [slice(i * HEAD, (i + 1) * HEAD) for i in range(step)]
    scored, weighed = [None] * step, [None] * step

    def score(i):
        scored[i] = score_stage(
            query[:, at[i]], grad_in[:, at[i]], latents[:total, at[i]], latents[total:, at[i]], factor[head + i]
        )

    def weigh(i):
        weighed[i] = weight_stage(scored[i][0], scored[i][1], allowed, scale)

    def project(i):
        weights_half, score_half = weighed[i]
        dot = lambda a, b, dims: lax.dot_general(a, b, dims, preferred_element_type=jnp.float32)
        query_part = dot(latents[:total, at[i]], score_half, TN) * scale
        query_out[:, at[i]] = jnp.transpose(query_part).astype(jnp.bfloat16)
        key_part = dot(score_half, query[:, at[i]], NN).astype(jnp.bfloat16)
        key_send[:, at[i]] = key_part[:256]
        key_keep[:, at[i]] = key_part[256:]
        value_part = dot(weights_half, scored[i][2], NN).astype(jnp.bfloat16)
        for slot, (out, row) in enumerate(((value_send, 0), (value_keep, 0), (value_send, 128), (value_keep, 128))):
            out[row : row + 128, at[i]] = value_part[slot * 128 : (slot + 1) * 128]

    score(0)
    for i in range(step):
        if i + 1 < step:
            score(i + 1)
        weigh(i)
        if i:
            project(i - 1)
    project(step - 1)


def attention(place, order, factor, seen, query, grad_in, key_own, value_own, pair, units, buffer, first, count, offset):
    tokens = query.shape[0]
    step = next(s for s in (4, 3, 2, 1) if count % s == first % s == offset % s == 0)
    width = step * HEAD
    scalar = pl.BlockSpec(memory_space=pltpu.SMEM)
    head_of = lambda h, place: (0, first // step + h)
    own_of = lambda h, place: (0, place[0] // step + first // step + h)
    part = lambda rows, at=0: pl.BlockSpec((rows, width), lambda h, place: (0, at // step + h))
    paired = lambda which: pl.BlockSpec((1, 128, width), lambda h, place: (which, 0, offset // step + h))
    if len(units) == 2:
        units = [u for u in units for _ in range(2)]
        unit_specs = [paired(0), paired(1)] * 2
    else:
        unit_specs = [part(128, offset)] * 4
    grads = jax.ShapeDtypeStruct((256, count * HEAD), jnp.bfloat16)
    grid_spec = pltpu.PrefetchScalarGridSpec(
        num_scalar_prefetch=1,
        grid=(count // step,),
        in_specs=[
            scalar,
            scalar,
            pl.BlockSpec((1, tokens), lambda h, place: (0, 0)),
            pl.BlockSpec((tokens, width), head_of),
            pl.BlockSpec((tokens, width), head_of),
            pl.BlockSpec((128, width), own_of),
            pl.BlockSpec((128, width), own_of),
            paired(0),
            paired(1),
        ]
        + unit_specs
        + [pl.BlockSpec(memory_space=pl.ANY)] * len(buffer),
        out_specs=[pl.BlockSpec((tokens, width), head_of)] + [part(256)] * 4,
        scratch_shapes=[pltpu.VMEM((1024, width), jnp.bfloat16)],
    )
    matmul = 2 * tokens * 512 * HEAD
    return pl.pallas_call(
        functools.partial(attention_body, first=first, scale=SCALE, step=step),
        grid_spec=grid_spec,
        out_shape=[jax.ShapeDtypeStruct(query.shape, jnp.bfloat16)] + [grads] * 4,
        input_output_aliases={14: 0} if buffer else {},
        compiler_params=pltpu.CompilerParams(dimension_semantics=("arbitrary",), vmem_limit_bytes=51 * 2**20),
        cost_estimate=pl.CostEstimate(
            flops=5 * count * matmul, transcendentals=count * tokens * 512, bytes_accessed=count * 2**20
        ),
        name="attention",
    )(place, order, factor, seen, query, grad_in, key_own, value_own, pair, pair, *units, *buffer)


def relabel(sizes, move):
    pairs = []
    total = math.prod(sizes)
    for source in range(total):
        rest, at = source, []
        for size in reversed(sizes):
            at.append(rest % size)
            rest //= size
        to = 0
        for index, size in zip(move(*reversed(at)), sizes):
            to = to * size + index % size
        pairs.append((source, to))
    return pairs


def columns(array, start, width):
    return lax.dynamic_slice(array, (0, start), (array.shape[0], width))


def shards(queries, visual_keys, visual_values, out_grad, gate_value, image_order, image_seen):
    query, grad_in, keys, values = queries[0], out_grad[0], visual_keys[0], visual_values[0]
    local = query.shape[1]
    heads = local // HEAD
    yh, c, x, _, z = (lax.axis_index(a) for a in AXES)
    colour = lambda x, z, c: (x + 2 * z) % 4 ^ c
    slot = lambda owner: 135 >> 2 * (owner ^ x) & 3
    row_block = lambda owner: slot(owner) * 128
    unit_at = lambda unit: unit // 2 * 512 + row_block((1 - yh) * 2 + unit % 2)
    own = yh * 2 + c
    pair_owner = yh * 2 + 1 - c
    place = [own * heads, row_block(own), 512 + row_block(own), row_block(pair_owner), 512 + row_block(pair_owner)]
    quarters = [unit_at(colour(x + dx, z + dz, c)) for dx, dz in ((0, 0), (3, 0), (1, 0), (0, 7))]
    halves = [unit_at(2 * kind + (x ^ c ^ away) % 2) for away in (0, 1) for kind in (0, 1)]
    images = [(x ^ flip) * 2 + half for flip in (2, 1, 3, 0) for half in (0, 1)]
    places = [jnp.stack(place + units + images).astype(jnp.int32) for units in (quarters, halves)]
    factor = jnp.tanh(gate_value[0])
    seen = image_seen[None]

    to_cross = relabel((2, 2, 4, 2), lambda yh, c, x, yl: (1 - yh, c ^ (x & 1), x, 1 - yl))
    flip_pairs = [(i, i ^ 1) for i in range(4)]
    cross_pairs = [(i, 3 - i) for i in range(4)]
    there = (1 - yh) * 2 + (c ^ (x & 1))
    wants_values = (x + 2 * z) % 4 // 2 == 1

    gathered = []
    first = 0
    shift = lambda array, axis, size, by: lax.ppermute(array, axis, [(i, (i + by) % size) for i in range(size)])
    for n, counts in enumerate(GATHERS):
        at, width = first * HEAD, sum(counts) * HEAD
        sent = [columns(a, there * local + at, width) for a in (keys, values)]
        sent = jnp.stack(sent) if n else jnp.where(wants_values, sent[1], sent[0])
        if n == 0:
            keys_too, values_too, sent = lax.optimization_barrier((keys, values, sent))
        pair = jnp.stack([columns(a, pair_owner * local + at, width) for a in (keys_too, values_too)])
        unit = lax.ppermute(sent, ("yh", "c", "x", "yl"), to_cross)
        pair = lax.ppermute(pair, "c", [(0, 1), (1, 0)])
        if n:
            units = [unit, lax.ppermute(unit, "x", flip_pairs)]
        else:
            units = [unit] + [shift(unit, *move) for move in (("x", 4, 1), ("x", 4, 3), ("z", 8, 1))]
        offset = 0
        for count in counts:
            gathered.append((places[n > 0], pair, units, first, count, offset))
            first += count
            offset += count

    buffer = ()
    ready, parts = [], []
    f32 = jnp.float32
    for place, pair, units, first, count, offset in gathered:
        whole, key_send, key_keep, value_send, value_keep = attention(
            place, image_order[0], factor, seen, query, grad_in, keys, values, pair, units,
            buffer, first, count, offset,
        )
        buffer = (whole,)
        mine = []
        for send, keep, near, far in (
            (key_send, key_keep, flip_pairs, cross_pairs), (value_send, value_keep, cross_pairs, flip_pairs)
        ):
            got = lax.ppermute(send, "x", near)
            passed = (keep[:128].astype(f32) + got[:128].astype(f32)).astype(jnp.bfloat16)
            passed = lax.ppermute(passed, "x", far)
            mine.append(
                (keep[128:].astype(f32) + got[128:].astype(f32) + passed.astype(f32)).astype(jnp.bfloat16)
            )
        ready.append(jnp.stack([m.reshape(16, 8, count * HEAD) for m in mine], axis=1))
    for members in PLANES:
        both = jnp.concatenate([ready[m] for m in members], axis=3)
        arrived = lax.all_to_all(both, ("yl", "z"), split_axis=0, concat_axis=0, tiled=True)
        parts.append(arrived.astype(f32).sum(axis=0))
    result = jnp.concatenate(parts, axis=2)
    return whole[None], result[0][None] * SCALE, result[1][None]


def solution(mesh):
    torus = Mesh(mesh.devices.reshape(2, 2, 4, 2, 8), AXES)
    img, txt = ("yh", "c"), ("x", "yl", "z")
    placed = (
        P(None, txt, img),
        P(None, img, None),
        P(None, img, None),
        P(None, txt, img),
        P(None, img),
        P(),
        P(txt),
    )
    return jax.shard_map(shards, mesh=torus, in_specs=placed, out_specs=(P(None, txt, img),) * 3, check_vma=False)
```

```python
import functools
import math

import jax
import jax.numpy as jnp
from jax import lax
from jax.experimental import pallas as pl
from jax.experimental.pallas import tpu as pltpu
from jax.sharding import Mesh, PartitionSpec as P


HEAD = 128
NT = (((1,), (1,)), ((), ()))
NN = (((1,), (0,)), ((), ()))
TN = (((0,), (0,)), ((), ()))
LOG2E = math.log2(math.e)
SCALE = 1.0 / math.sqrt(HEAD)
GATHERS = ((8,), (8,))
PLANES = ((0,), (1,))
AXES = ("yh", "c", "x", "yl", "z")


def score_stage(query, grad_in, keys, values, factor):
    gated = (grad_in.astype(jnp.float32) * factor).astype(jnp.bfloat16)
    scores = lax.dot_general(keys, query, NT, preferred_element_type=jnp.float32)
    weight_grad = lax.dot_general(values, gated, NT, preferred_element_type=jnp.float32)
    return scores, weight_grad, gated


def by_eights(op, blocks):
    folded = [op(b.reshape(-1, 8, b.shape[1]), axis=0) for b in blocks]
    return functools.reduce(jnp.maximum if op is jnp.max else jnp.add, folded)


def weight_stage(scores, weight_grad, allowed, scale):
    block = scores.shape[0] // len(allowed)
    cut = lambda array: [array[b * block : (b + 1) * block] for b in range(len(allowed))]
    masked = [jnp.where(a, s, -1e30) for a, s in zip(allowed, cut(scores))]
    grads = cut(weight_grad)
    top = jnp.max(by_eights(jnp.max, masked), axis=0, keepdims=True)
    exponent = [jnp.exp2((m - top) * (scale * LOG2E)) for m in masked]
    share = 1.0 / jnp.sum(by_eights(jnp.sum, exponent), axis=0, keepdims=True)
    crossed = by_eights(jnp.sum, [e * g for e, g in zip(exponent, grads)])
    row_delta = jnp.sum(crossed, axis=0, keepdims=True) * share
    weights = [e * share for e in exponent]
    weights_half = jnp.concatenate([w.astype(jnp.bfloat16) for w in weights], axis=0)
    score_half = jnp.concatenate(
        [(w * (g - row_delta)).astype(jnp.bfloat16) for w, g in zip(weights, grads)], axis=0
    )
    return weights_half, score_half


def attention_body(
    place, order, factor, seen, query, grad_in, key_own, value_own, key_pair, value_pair,
    unit_0, unit_1, unit_2, unit_3, *rest, first, scale, step,
):
    query_out, key_send, key_keep, value_send, value_keep, latents = rest[-6:]
    head = first + pl.program_id(0) * step
    sources = (key_own, value_own, key_pair, value_pair, unit_0, unit_1, unit_2, unit_3)
    for i, source in enumerate(sources):
        latents[pl.ds(pl.multiple_of(place[1 + i], 128), 128), :] = source[...].reshape(128, step * HEAD)
    allowed = [order[place[9 + b]] < seen[...] for b in range(8)]
    total = latents.shape[0] // 2
    at = [slice(i * HEAD, (i + 1) * HEAD) for i in range(step)]
    scored, weighed = [None] * step, [None] * step

    def score(i):
        scored[i] = score_stage(
            query[:, at[i]], grad_in[:, at[i]], latents[:total, at[i]], latents[total:, at[i]], factor[head + i]
        )

    def weigh(i):
        weighed[i] = weight_stage(scored[i][0], scored[i][1], allowed, scale)

    def project(i):
        weights_half, score_half = weighed[i]
        dot = lambda a, b, dims: lax.dot_general(a, b, dims, preferred_element_type=jnp.float32)
        query_part = dot(latents[:total, at[i]], score_half, TN) * scale
        query_out[:, at[i]] = jnp.transpose(query_part).astype(jnp.bfloat16)
        key_part = dot(score_half, query[:, at[i]], NN).astype(jnp.bfloat16)
        key_send[:, at[i]] = key_part[:256]
        key_keep[:, at[i]] = key_part[256:]
        value_part = dot(weights_half, scored[i][2], NN).astype(jnp.bfloat16)
        for slot, (out, row) in enumerate(((value_send, 0), (value_keep, 0), (value_send, 128), (value_keep, 128))):
            out[row : row + 128, at[i]] = value_part[slot * 128 : (slot + 1) * 128]

    score(0)
    for i in range(step):
        if i + 1 < step:
            score(i + 1)
        weigh(i)
        if i:
            project(i - 1)
    project(step - 1)


def attention(place, order, factor, seen, query, grad_in, key_own, value_own, pair, units, buffer, first, count, offset):
    tokens = query.shape[0]
    step = next(s for s in (4, 3, 2, 1) if count % s == first % s == offset % s == 0)
    width = step * HEAD
    scalar = pl.BlockSpec(memory_space=pltpu.SMEM)
    head_of = lambda h, place: (0, first // step + h)
    own_of = lambda h, place: (0, place[0] // step + first // step + h)
    part = lambda rows, at=0: pl.BlockSpec((rows, width), lambda h, place: (0, at // step + h))
    paired = lambda which: pl.BlockSpec((1, 128, width), lambda h, place: (which, 0, offset // step + h))
    grads = jax.ShapeDtypeStruct((256, count * HEAD), jnp.bfloat16)
    grid_spec = pltpu.PrefetchScalarGridSpec(
        num_scalar_prefetch=1,
        grid=(count // step,),
        in_specs=[
            scalar,
            scalar,
            pl.BlockSpec((1, tokens), lambda h, place: (0, 0)),
            pl.BlockSpec((tokens, width), head_of),
            pl.BlockSpec((tokens, width), head_of),
            pl.BlockSpec((128, width), own_of),
            pl.BlockSpec((128, width), own_of),
            paired(0),
            paired(1),
        ]
        + [part(128, offset)] * 4
        + [pl.BlockSpec(memory_space=pl.ANY)] * len(buffer),
        out_specs=[pl.BlockSpec((tokens, width), head_of)] + [part(256)] * 4,
        scratch_shapes=[pltpu.VMEM((1024, width), jnp.bfloat16)],
    )
    matmul = 2 * tokens * 512 * HEAD
    return pl.pallas_call(
        functools.partial(attention_body, first=first, scale=SCALE, step=step),
        grid_spec=grid_spec,
        out_shape=[jax.ShapeDtypeStruct(query.shape, jnp.bfloat16)] + [grads] * 4,
        input_output_aliases={14: 0} if buffer else {},
        compiler_params=pltpu.CompilerParams(dimension_semantics=("arbitrary",), vmem_limit_bytes=49 * 2**20),
        cost_estimate=pl.CostEstimate(
            flops=5 * count * matmul, transcendentals=count * tokens * 512, bytes_accessed=count * 2**20
        ),
        name="attention",
    )(place, order, factor, seen, query, grad_in, key_own, value_own, pair, pair, *units, *buffer)


def relabel(sizes, move):
    pairs = []
    total = math.prod(sizes)
    for source in range(total):
        rest, at = source, []
        for size in reversed(sizes):
            at.append(rest % size)
            rest //= size
        to = 0
        for index, size in zip(move(*reversed(at)), sizes):
            to = to * size + index % size
        pairs.append((source, to))
    return pairs


def columns(array, start, width):
    return lax.dynamic_slice(array, (0, start), (array.shape[0], width))


def shards(queries, visual_keys, visual_values, out_grad, gate_value, image_order, image_seen):
    query, grad_in, keys, values = queries[0], out_grad[0], visual_keys[0], visual_values[0]
    local = query.shape[1]
    heads = local // HEAD
    yh, c, x, _, z = (lax.axis_index(a) for a in AXES)
    colour = lambda x, z, c: (x + 2 * z) % 4 ^ c
    slot = lambda owner: 135 >> 2 * (owner ^ x) & 3
    row_block = lambda owner: slot(owner) * 128
    unit_at = lambda unit: unit // 2 * 512 + row_block((1 - yh) * 2 + unit % 2)
    own = yh * 2 + c
    pair_owner = yh * 2 + 1 - c
    place = [own * heads, row_block(own), 512 + row_block(own), row_block(pair_owner), 512 + row_block(pair_owner)]
    place += [unit_at(colour(x + dx, z + dz, c)) for dx, dz in ((0, 0), (3, 0), (1, 0), (0, 7))]
    place += [(x ^ flip) * 2 + half for flip in (2, 1, 3, 0) for half in (0, 1)]
    place = jnp.stack(place).astype(jnp.int32)
    factor = jnp.tanh(gate_value[0])
    seen = image_seen[None]

    to_cross = relabel((2, 2, 4, 2), lambda yh, c, x, yl: (1 - yh, c ^ (x & 1), x, 1 - yl))
    flip_pairs = [(i, i ^ 1) for i in range(4)]
    cross_pairs = [(i, 3 - i) for i in range(4)]
    there = (1 - yh) * 2 + (c ^ (x & 1))
    wants_values = (x + 2 * z) % 4 // 2 == 1

    gathered = []
    first = 0
    for n, counts in enumerate(GATHERS):
        at, width = first * HEAD, sum(counts) * HEAD
        sent = [columns(a, there * local + at, width) for a in (keys, values)]
        sent = jnp.where(wants_values, sent[1], sent[0])
        if n == 0:
            keys_too, values_too, sent = lax.optimization_barrier((keys, values, sent))
        pair = jnp.stack([columns(a, pair_owner * local + at, width) for a in (keys_too, values_too)])
        unit = lax.ppermute(sent, ("yh", "c", "x", "yl"), to_cross)
        pair = lax.ppermute(pair, "c", [(0, 1), (1, 0)])
        units = [unit]
        for axis, size, by in (("x", 4, 1), ("x", 4, 3), ("z", 8, 1)):
            units.append(lax.ppermute(unit, axis, [(i, (i + by) % size) for i in range(size)]))
        offset = 0
        for count in counts:
            gathered.append((pair, units, first, count, offset))
            first += count
            offset += count

    buffer = ()
    ready, parts = [], []
    f32 = jnp.float32
    for pair, units, first, count, offset in gathered:
        whole, key_send, key_keep, value_send, value_keep = attention(
            place, image_order[0], factor, seen, query, grad_in, keys, values, pair, units,
            buffer, first, count, offset,
        )
        buffer = (whole,)
        mine = []
        for send, keep, near, far in (
            (key_send, key_keep, flip_pairs, cross_pairs), (value_send, value_keep, cross_pairs, flip_pairs)
        ):
            got = lax.ppermute(send, "x", near)
            passed = (keep[:128].astype(f32) + got[:128].astype(f32)).astype(jnp.bfloat16)
            passed = lax.ppermute(passed, "x", far)
            mine.append(
                (keep[128:].astype(f32) + got[128:].astype(f32) + passed.astype(f32)).astype(jnp.bfloat16)
            )
        ready.append(jnp.stack([m.reshape(16, 8, count * HEAD) for m in mine], axis=1))
    for members in PLANES:
        both = jnp.concatenate([ready[m] for m in members], axis=3)
        arrived = lax.all_to_all(both, ("yl", "z"), split_axis=0, concat_axis=0, tiled=True)
        parts.append(arrived.astype(f32).sum(axis=0))
    result = jnp.concatenate(parts, axis=2)
    return whole[None], result[0][None] * SCALE, result[1][None]


def solution(mesh):
    torus = Mesh(mesh.devices.reshape(2, 2, 4, 2, 8), AXES)
    img, txt = ("yh", "c"), ("x", "yl", "z")
    placed = (
        P(None, txt, img),
        P(None, img, None),
        P(None, img, None),
        P(None, txt, img),
        P(None, img),
        P(),
        P(txt),
    )
    return jax.shard_map(shards, mesh=torus, in_specs=placed, out_specs=(P(None, txt, img),) * 3, check_vma=False)
```
